256 devices in a mesh: src: 8 (over y, core), dst: 32 (over z, x).
Axes of the slice: x: 4, y: 4, z: 8, core: 2. Of those that a mesh axis runs over, the one named last changes fastest.
Arguments:
- features: bfloat16 [65536, 768], P(('src', 'dst')), may hold values from -6 to 6
- edge_tiles: bfloat16 [8, 32, 64, 128, 128], P('src', 'dst'), may hold values from -0.3125 to 0.3125
- tile_src: int32 [8, 32, 64], P('src', 'dst'), may hold values from 0 to 15
- tile_dst: int32 [8, 32, 64], P('src', 'dst'), may hold values from 0 to 63, as said below
- tile_count: int32 [8, 32], P('src', 'dst'), may hold values from 1 to 64, as said below
- weight: bfloat16 [768, 1024], replicated, may hold values from -0.21875 to 0.21875
- out_bias: float32 [1024], replicated, may hold values from -3 to 3
- out_grad: bfloat16 [65536, 1024], P(('src', 'dst')), may hold values from -24 to 24
Outputs:
- hidden: bfloat16 [65536, 1024], P(('src', 'dst'))
- feature_grad: bfloat16 [65536, 768], P(('src', 'dst'))
- weight_grad: float32 [768, 1024], replicated
- bias_grad: float32 [1024], replicated
The draws below stay inside these ranges and needn't reach their ends.
Inputs may be any that keep to these rules, and one draw needn't show every extreme that they name: `tile_src`: block s of the source column of device (i, k) is block s % 2 of device (s // 2, k). `tile_dst`: block e of the destination row of device (i, k) is block e % 2 of device (i, e // 2). On one device, all tile slots whose destination blocks lie on one device name the same block. In every row of devices, slot 0 of every device names one common block. `tile_count`: some device uses all 64 slots.
All inputs are finite; a program needn't handle non-finite values.
Results may differ from the reference program's by a relative error of at most 0.024.
Values may be sent and summed in bfloat16 or wider, within the bound.
No kernel may reach another device: no remote copies, remote signals or barrier semaphores. Data moves between devices by JAX's collectives and lax.ppermute only.
A program may use at most 128 MiB of HBM per device.

```python
import jax
import jax.numpy as jnp
from jax import lax

F = 768
H = 1024
TILE = 128
BLK_DEV = 2
TILE_CAP = 64
NODES = 65536
N_SRC = 8
N_DST = 32


def draw_tile_dst(key, part):
    keys = jax.random.split(jax.random.fold_in(key, 7), 5)
    hub_master = jax.random.randint(keys[0], (N_SRC,), 0, N_DST)
    hub_block = jax.random.randint(keys[1], (N_SRC,), 0, BLK_DEV)
    table = jax.random.randint(keys[2], (N_SRC, N_DST, N_DST), 0, BLK_DEV)
    is_hub = jnp.arange(N_DST)[None, None, :] == hub_master[:, None, None]
    table = jnp.where(is_hub, hub_block[:, None, None], table)
    toward_hub = jax.random.randint(keys[3], (N_SRC, N_DST, TILE_CAP), 0, 2)
    others = jax.random.randint(keys[4], (N_SRC, N_DST, TILE_CAP), 0, N_DST)
    master = jnp.where(toward_hub == 1, hub_master[:, None, None], others)
    master = master.at[:, :, 0].set(jnp.broadcast_to(hub_master[:, None], (N_SRC, N_DST)))
    chosen = jnp.take_along_axis(table, master, axis=2)
    return (master * BLK_DEV + chosen).astype(jnp.int32)


def draw_tile_count(key, part):
    keys = jax.random.split(jax.random.fold_in(key, 11), 4)
    base_count = jax.random.randint(keys[0], (N_SRC, N_DST), 1, max(2, TILE_CAP // 2))
    heavy = jax.random.randint(keys[1], (N_SRC, N_DST), 0, 8) == 0
    large_count = jax.random.randint(keys[2], (N_SRC, N_DST), TILE_CAP // 2, TILE_CAP + 1)
    counts = jnp.where(heavy, large_count, base_count).reshape(N_SRC * N_DST)
    chosen_spot = jax.random.randint(keys[3], (), 0, N_SRC * N_DST)
    counts = counts.at[chosen_spot].set(TILE_CAP)
    return counts.reshape(N_SRC, N_DST).astype(jnp.int32)


def set_ends(values, rng, least, largest):
    index_at = [jax.random.randint(jax.random.fold_in(rng, axis), (), 0, length) for axis, length in enumerate(values.shape)]
    main_axis = values.shape.index(max(values.shape))
    beside = index_at[:main_axis] + [(index_at[main_axis] + 1) % values.shape[main_axis]] + index_at[main_axis + 1:]
    return values.at[tuple(index_at)].set(least).at[tuple(beside)].set(largest)


def raised(result, stream_key, source, target, parts, factor):
    def block_of(dim):
        return (jnp.arange(result.shape[dim]) // (result.shape[dim] // parts)).reshape((-1,) + (1,) * (result.ndim - 1 - dim))

    one_side = jax.random.permutation(stream_key, parts)[block_of(target)]
    other_side = (block_of(target) + parts // 2) % parts
    return jnp.where((block_of(source) == one_side) | (block_of(source) == other_side), factor * result, result)


def block_levels(stream_key, shape, shards, low, high):
    gain = 1.0
    for position, blocks in shards:
        heights = jax.random.uniform(jax.random.fold_in(jax.random.fold_in(stream_key, 6), position), (blocks,), jnp.float32, low / len(shards), high / len(shards))
        gain = gain * jnp.repeat(jnp.exp(heights), shape[position] // blocks).reshape((-1,) + (1,) * (len(shape) - 1 - position))
    return gain


def gaussian(own_key, dims, width, most, shards=(), kind=jnp.bfloat16):
    drawn = jax.random.normal(own_key, dims, jnp.float32) * width
    if len(shards) > 0:
        drawn = block_levels(own_key, dims, shards, -0.22, 0.18) * drawn
    return jnp.clip(drawn, min=-most, max=most).astype(kind)


def bell_draw_with(own_key, shape, width, bound, cuts, heavy, kind=jnp.bfloat16):
    entries = width * jax.random.normal(own_key, shape, jnp.float32)
    if cuts:
        entries = entries * block_levels(own_key, shape, cuts, -0.22, 0.18)
    return jnp.clip(raised(entries, jax.random.fold_in(own_key, 3), *heavy), -bound, bound).astype(kind)


def setup_inputs(seed: int = 0) -> dict:
    streams_of = jax.random.split(jax.random.key(seed), 9)
    return {
        "features": gaussian(streams_of[0], (NODES, F), 1.0, 6.0, ((0, 256),)),
        "edge_tiles": gaussian(streams_of[1], (N_SRC, N_DST, TILE_CAP, TILE, TILE), (3 * TILE) ** -0.5, 0.3125, ((0, 8), (1, 32))),
        "tile_src": set_ends(jax.random.randint(streams_of[2], (N_SRC, N_DST, TILE_CAP), 0, N_SRC * BLK_DEV), jax.random.fold_in(streams_of[2], 1), 0, (N_SRC * BLK_DEV) - 1).astype(jnp.int32),
        "tile_dst": draw_tile_dst(jax.random.fold_in(streams_of[8], 71), 0),
        "tile_count": draw_tile_count(jax.random.fold_in(streams_of[8], 71), 0),
        "weight": gaussian(streams_of[5], (F, H), F ** -0.5, 0.21875),
        "out_bias": gaussian(streams_of[6], (H,), 0.5, 3.0, (), jnp.float32),
        "out_grad": bell_draw_with(streams_of[7], (NODES, H), 1.0, 24.0, ((0, 256),), (0, 1, 256, 6.0)),
    }


def reference(features, edge_tiles, tile_src, tile_dst, tile_count, weight, out_bias, out_grad):
    capacity = edge_tiles.shape[2]
    col_blocks = N_SRC * BLK_DEV
    row_blocks = N_DST * BLK_DEV
    blocked = features.reshape(N_SRC, N_DST, BLK_DEV, TILE, F)
    slot_ids = jnp.arange(capacity, dtype=jnp.int32)
    device_ids = jnp.arange(N_SRC * N_DST, dtype=jnp.int32)

    def forward_step(aggregate, device_index):
        src_index = device_index // N_DST
        dst_index = device_index % N_DST
        adjacency = edge_tiles[src_index, dst_index].astype(jnp.float32)
        column = blocked[:, dst_index].reshape(col_blocks, TILE, F)
        picked = column[tile_src[src_index, dst_index]].astype(jnp.float32)
        alive_mask = (slot_ids < tile_count[src_index, dst_index]).astype(jnp.float32)
        partial_value = jnp.einsum("tij,tjf->tif", adjacency, picked) * alive_mask[:, None, None]
        summed = jnp.zeros((row_blocks, TILE, F), jnp.float32).at[tile_dst[src_index, dst_index]].add(partial_value)
        rounded = lax.optimization_barrier(summed.astype(jnp.bfloat16)).astype(jnp.float32)
        return aggregate.at[src_index].add(rounded.reshape(N_DST, BLK_DEV, TILE, F)), None

    start_agg = jnp.zeros((N_SRC, N_DST, BLK_DEV, TILE, F), jnp.float32)
    aggregate, _ = lax.scan(forward_step, start_agg, device_ids)
    agg_rows = aggregate.reshape(NODES, F).astype(jnp.bfloat16)
    preact = jnp.dot(agg_rows, weight, preferred_element_type=jnp.float32) + out_bias
    gate_value = jax.nn.sigmoid(preact)
    hidden = (preact * gate_value).astype(jnp.bfloat16)
    pre_grad = out_grad.astype(jnp.float32) * (gate_value * (1.0 + preact * (1.0 - gate_value)))
    pre_grad_b = pre_grad.astype(jnp.bfloat16)
    weight_grad = jnp.dot(agg_rows.T, pre_grad_b, preferred_element_type=jnp.float32)
    bias_grad = jnp.sum(pre_grad, axis=0)
    back = jnp.dot(pre_grad_b, weight.T, preferred_element_type=jnp.float32).astype(jnp.bfloat16)
    grad_rows = back.reshape(N_SRC, row_blocks, TILE, F)

    def backward_step(grad_total, device_index):
        src_index = device_index // N_DST
        dst_index = device_index % N_DST
        adjacency = edge_tiles[src_index, dst_index].astype(jnp.float32)
        wanted = grad_rows[src_index][tile_dst[src_index, dst_index]].astype(jnp.float32)
        alive_mask = (slot_ids < tile_count[src_index, dst_index]).astype(jnp.float32)
        source = jnp.einsum("tji,tjf->tif", adjacency, wanted) * alive_mask[:, None, None]
        summed = jnp.zeros((col_blocks, TILE, F), jnp.float32).at[tile_src[src_index, dst_index]].add(source)
        rounded = lax.optimization_barrier(summed.astype(jnp.bfloat16)).astype(jnp.float32)
        return grad_total.at[:, dst_index].add(rounded.reshape(N_SRC, BLK_DEV, TILE, F)), None

    start_grad = jnp.zeros((N_SRC, N_DST, BLK_DEV, TILE, F), jnp.float32)
    grad_total, _ = lax.scan(backward_step, start_grad, device_ids)
    feature_grad = grad_total.reshape(NODES, F).astype(jnp.bfloat16)
    return (hidden, feature_grad, weight_grad, bias_grad)
```

```python
import functools

import jax
import jax.numpy as jnp
from jax import lax
from jax.experimental import pallas as pl
from jax.experimental.pallas import tpu as pltpu
from jax.sharding import Mesh
from jax.sharding import PartitionSpec as P

SRC = ("y", "c")
DST = ("z", "x")
ALL = ("y", "c", "z", "x")
CHUNKS = 2
SMEM = pl.BlockSpec(memory_space=pltpu.SMEM)
VMEM = pl.BlockSpec(memory_space=pltpu.VMEM)


def link_tiles(key_of, count, head, nxt, groups):
    def clear(g, _):
        head[g] = -1
        return 0

    lax.fori_loop(0, groups, clear, 0)

    def push(t, _):
        g = key_of(t)
        nxt[t] = head[g]
        head[g] = t
        return 0

    lax.fori_loop(0, count, push, 0)


def walk(head, nxt, g, pair, acc):
    def one(t):
        t2 = nxt[t]
        has = t2 >= 0
        t2 = jnp.maximum(t2, 0)
        return pair(t, t2, has), jnp.where(has, nxt[t2], -1)

    value, t = one(head[g])
    acc[...] = value

    def more(t):
        value, t = one(t)
        acc[...] += value
        return t

    lax.while_loop(lambda t: t >= 0, more, t)


def forward_kernel(src, dst, count, adj, col, *rest, blocks, nx, chunks):
    outs, (head, nxt, acc) = rest[:chunks], rest[chunks:]
    nz = outs[0].shape[1]
    rows = outs[0].shape[2]
    link_tiles(lambda t: dst[t] // blocks, count[0], head, nxt, nx * nz)

    def pair(t, t2, has):
        second = adj[t2]
        second = jnp.where(has, second, jnp.zeros_like(second))
        left = jnp.concatenate([adj[t], second], axis=1)
        right = jnp.concatenate([col[src[t]], col[src[t2]]], axis=0)
        return jnp.dot(left, right, preferred_element_type=jnp.float32)

    def master(m, _):
        xi = lax.rem(m, nx)
        zi = m // nx

        @pl.when(head[m] < 0)
        def _():
            for out in outs:
                out[xi, zi] = jnp.zeros(out.shape[2:], out.dtype)

        @pl.when(head[m] >= 0)
        def _():
            walk(head, nxt, m, pair, acc)
            for r, out in enumerate(outs):
                out[xi, zi] = acc[r * rows : (r + 1) * rows].astype(out.dtype)

        return 0

    lax.fori_loop(0, nx * nz, master, 0)


def forward_products(src_ids, dst_ids, count, adj, col, blocks, nx, nz, chunks):
    tiles, size, _ = adj.shape
    width = col.shape[2]
    rows = size // chunks
    return pl.pallas_call(
        functools.partial(forward_kernel, blocks=blocks, nx=nx, chunks=chunks),
        out_shape=[jax.ShapeDtypeStruct((nx, nz, rows, width), jnp.bfloat16)] * chunks,
        in_specs=[SMEM, SMEM, SMEM, VMEM, VMEM],
        out_specs=[VMEM] * chunks,
        scratch_shapes=[
            pltpu.SMEM((nx * nz,), jnp.int32),
            pltpu.SMEM((tiles,), jnp.int32),
            pltpu.VMEM((size, width), jnp.float32),
        ],
        compiler_params=pltpu.CompilerParams(vmem_limit_bytes=48 * 1024 * 1024),
        cost_estimate=pl.CostEstimate(
            flops=2 * tiles * size * size * width, transcendentals=0, bytes_accessed=12_000_000
        ),
        name="forward_products",
    )(src_ids, dst_ids, count, adj, col)


def backward_kernel(src, dst, count, adj, *rest, blocks, nx, chunks):
    wanted, out, (head, nxt, acc) = rest[:chunks], rest[chunks], rest[chunks + 1 :]
    groups = out.shape[0]
    link_tiles(lambda t: src[t], count[0], head, nxt, groups)

    def rows_of(t):
        m = dst[t] // blocks
        xi = lax.rem(m, nx)
        zi = m // nx
        return [w[xi, zi] for w in wanted]

    def pair(t, t2, has):
        second = adj[t2]
        second = jnp.where(has, second, jnp.zeros_like(second))
        left = jnp.concatenate([adj[t], second], axis=0)
        right = jnp.concatenate(rows_of(t) + rows_of(t2), axis=0)
        return lax.dot_general(
            left, right, (((0,), (0,)), ((), ())), preferred_element_type=jnp.float32
        )

    def block(s, _):
        @pl.when(head[s] < 0)
        def _():
            out[s] = jnp.zeros(out.shape[1:], out.dtype)

        @pl.when(head[s] >= 0)
        def _():
            walk(head, nxt, s, pair, acc)
            out[s] = acc[...].astype(out.dtype)

        return 0

    lax.fori_loop(0, groups, block, 0)


def backward_products(src_ids, dst_ids, count, adj, wanted, blocks, groups):
    tiles, size, _ = adj.shape
    nx, _, _, width = wanted[0].shape
    chunks = len(wanted)
    return pl.pallas_call(
        functools.partial(backward_kernel, blocks=blocks, nx=nx, chunks=chunks),
        out_shape=jax.ShapeDtypeStruct((groups, size, width), jnp.bfloat16),
        in_specs=[SMEM, SMEM, SMEM, VMEM] + [VMEM] * chunks,
        out_specs=VMEM,
        scratch_shapes=[
            pltpu.SMEM((groups,), jnp.int32),
            pltpu.SMEM((tiles,), jnp.int32),
            pltpu.VMEM((size, width), jnp.float32),
        ],
        compiler_params=pltpu.CompilerParams(vmem_limit_bytes=48 * 1024 * 1024),
        cost_estimate=pl.CostEstimate(
            flops=2 * tiles * size * size * width, transcendentals=0, bytes_accessed=12_000_000
        ),
        name="backward_products",
    )(src_ids, dst_ids, count, adj, *wanted)


def combine_kernel(asked, arrived, out):
    z = pl.program_id(0)
    nx = arrived.shape[0]
    values = [arrived[x, 0].astype(jnp.float32) for x in range(nx)]
    for j in range(out.shape[1]):
        total = jnp.zeros(values[0].shape, jnp.float32)
        for x in range(nx):
            total += jnp.where(asked[x, z] == j, values[x], 0.0)
        out[0, j] = total.astype(out.dtype)


def combine(asked, arrived, blocks):
    nx, nz, rows, width = arrived.shape
    return pl.pallas_call(
        combine_kernel,
        grid=(nz,),
        out_shape=jax.ShapeDtypeStruct((nz, blocks, rows, width), jnp.bfloat16),
        in_specs=[SMEM, pl.BlockSpec((nx, 1, rows, width), lambda z: (0, z, 0, 0))],
        out_specs=pl.BlockSpec((1, blocks, rows, width), lambda z: (z, 0, 0, 0)),
        cost_estimate=pl.CostEstimate(
            flops=8 * nx * nz * rows * width, transcendentals=0, bytes_accessed=6_000_000
        ),
        name="combine",
    )(asked, arrived)


def pick_kernel(asked, held, out):
    z = pl.program_id(0)
    for x in range(out.shape[0]):
        out[x, 0] = held[0, asked[x, z]]


def pick(asked, held, nx):
    nz, blocks, rows, width = held.shape
    return pl.pallas_call(
        pick_kernel,
        grid=(nz,),
        out_shape=jax.ShapeDtypeStruct((nx, nz, rows, width), jnp.bfloat16),
        in_specs=[SMEM, pl.BlockSpec((1, blocks, rows, width), lambda z: (z, 0, 0, 0))],
        out_specs=pl.BlockSpec((nx, 1, rows, width), lambda z: (0, z, 0, 0)),
        cost_estimate=pl.CostEstimate(
            flops=nx * nz * rows * width, transcendentals=0, bytes_accessed=6_000_000
        ),
        name="pick",
    )(asked, held)


def reduced_grads(weight_term, bias_term):
    feat, hidden = weight_term.shape
    src = lax.axis_size(SRC)
    dst = lax.axis_size(DST)
    part = feat // src // dst
    own = lax.psum_scatter(
        weight_term.astype(jnp.bfloat16), SRC, scatter_dimension=0, tiled=True
    )
    bias = bias_term.astype(jnp.bfloat16).reshape(dst, 1, hidden // dst)
    bias = jnp.pad(bias, ((0, 0), (0, 0), (0, hidden - hidden // dst)))
    lines = jnp.concatenate([own.reshape(dst, part, hidden), bias], axis=1)
    arrived = lax.all_to_all(lines, DST, 0, 0, tiled=True)
    summed = jnp.sum(arrived.astype(jnp.float32), axis=0).astype(jnp.bfloat16)
    shared = lax.all_to_all(
        jnp.broadcast_to(summed[None], (dst, *summed.shape)), DST, 0, 0, tiled=True
    )
    mine = shared[:, :part].reshape(dst * part, hidden)
    bias = shared[:, part, : hidden // dst].reshape(1, hidden)
    mine = jnp.concatenate([mine, jnp.pad(bias, ((0, 15), (0, 0)))], axis=0)
    whole = lax.all_gather(mine, SRC, axis=0).astype(jnp.float32)
    weight_grad = whole[:, : dst * part].reshape(feat, hidden)
    return weight_grad, jnp.sum(whole[:, dst * part], axis=0)


def per_device(features, edge_tiles, tile_src, tile_dst, tile_count, weight, out_bias, out_grad):
    capacity, size = edge_tiles.shape[2:4]
    block_rows, feat_width = features.shape
    blocks = block_rows // size
    nx, nz = lax.axis_size("x"), lax.axis_size("z")
    masters = nx * nz
    holders = lax.axis_size(SRC)
    rows = size // CHUNKS
    adj = edge_tiles.reshape(capacity, size, size)
    src_ids = tile_src.reshape(capacity)
    dst_ids = tile_dst.reshape(capacity)
    count = tile_count.reshape(1)

    alive = jnp.arange(capacity, dtype=jnp.int32) < count[0]
    routing = (dst_ids // blocks)[None, :] == jnp.arange(masters, dtype=jnp.int32)[:, None]
    inner = jnp.where(routing & alive[None, :], (dst_ids % blocks)[None, :], 0)
    wanted = jnp.max(inner, axis=1).reshape(nz, nx).T
    asked = lax.all_to_all(
        jnp.broadcast_to(wanted[:, :, None], (nx, nz, 128)), "x", 0, 0, tiled=True
    )[:, :, 0]

    column = lax.all_gather(features, SRC, axis=0, tiled=True)
    column = column.reshape(holders * blocks, size, feat_width)
    outgoing = forward_products(
        src_ids, dst_ids, count, adj, column, blocks, nx, nz, CHUNKS
    )

    grads = out_grad.reshape(blocks, size, -1)
    hidden, aggregates, pre_grads, bias_term, received = [], [], [], 0.0, []
    for r in range(CHUNKS):
        arrived = lax.all_to_all(outgoing[r], "x", 0, 0, tiled=True)
        merged = combine(asked, arrived, blocks)
        aggregate = lax.psum_scatter(
            merged.reshape(nz * blocks * rows, feat_width), "z", scatter_dimension=0, tiled=True
        )
        preact = jnp.dot(aggregate, weight, preferred_element_type=jnp.float32) + out_bias
        gate = jax.nn.sigmoid(preact)
        hidden.append((preact * gate).astype(jnp.bfloat16).reshape(blocks, rows, -1))
        grad_in = grads[:, r * rows : (r + 1) * rows].reshape(blocks * rows, -1)
        pre_grad = grad_in.astype(jnp.float32) * (gate * (1.0 + preact * (1.0 - gate)))
        pre_grad_b = pre_grad.astype(jnp.bfloat16)
        bias_term += jnp.sum(pre_grad, axis=0)
        aggregates.append(aggregate)
        pre_grads.append(pre_grad_b)
        back = lax.dot_general(
            pre_grad_b, weight, (((1,), (1,)), ((), ())), preferred_element_type=jnp.float32
        ).astype(jnp.bfloat16)
        held = lax.all_gather(back, "z", axis=0, tiled=True)
        chosen = pick(asked, held.reshape(nz, blocks, rows, feat_width), nx)
        received.append(lax.all_to_all(chosen, "x", 0, 0, tiled=True))

    weight_term = lax.dot_general(
        jnp.concatenate(aggregates, axis=0),
        jnp.concatenate(pre_grads, axis=0),
        (((0,), (0,)), ((), ())),
        preferred_element_type=jnp.float32,
    )
    weight_grad, bias_grad = reduced_grads(weight_term, bias_term)

    source = backward_products(
        src_ids, dst_ids, count, adj, received, blocks, holders * blocks
    )
    feature_grad = lax.psum_scatter(
        source.reshape(holders * block_rows, feat_width), SRC, scatter_dimension=0, tiled=True
    )
    hidden = jnp.concatenate(hidden, axis=1).reshape(block_rows, -1)
    return (hidden, feature_grad, weight_grad, bias_grad)


def solution(mesh):
    split = Mesh(mesh.devices.reshape(4, 2, 8, 4), ALL)
    in_specs = (
        P(ALL, None),
        P(SRC, DST, None, None, None),
        P(SRC, DST, None),
        P(SRC, DST, None),
        P(SRC, DST),
        P(),
        P(),
        P(ALL, None),
    )
    out_specs = (P(ALL, None), P(ALL, None), P(), P())
    return jax.shard_map(
        per_device, mesh=split, in_specs=in_specs, out_specs=out_specs, check_vma=False
    )
```

```python
import functools

import jax
import jax.numpy as jnp
from jax import lax
from jax.experimental import pallas as pl
from jax.experimental.pallas import tpu as pltpu
from jax.sharding import Mesh
from jax.sharding import PartitionSpec as P

SRC = ("y", "c")
DST = ("z", "x")
ALL = ("y", "c", "z", "x")
CHUNK_ROWS = (48, 48, 32)
SMEM = pl.BlockSpec(memory_space=pltpu.SMEM)
VMEM = pl.BlockSpec(memory_space=pltpu.VMEM)
HBM = pl.BlockSpec(memory_space=pltpu.HBM)


def link_tiles(key_of, count, head, nxt, groups):
    def clear(g, _):
        head[g] = -1
        return 0

    lax.fori_loop(0, groups, clear, 0)

    def push(t, _):
        g = key_of(t)
        nxt[t] = head[g]
        head[g] = t
        return 0

    lax.fori_loop(0, count, push, 0)


def walk(head, nxt, g, pair, acc):
    def one(t):
        t2 = nxt[t]
        has = t2 >= 0
        t2 = jnp.maximum(t2, 0)
        return pair(t, t2, has), jnp.where(has, nxt[t2], -1)

    value, t = one(head[g])
    acc[...] = value

    def more(t):
        value, t = one(t)
        acc[...] += value
        return t

    lax.while_loop(lambda t: t >= 0, more, t)


def starts_of(chunk_rows):
    return [sum(chunk_rows[:r]) for r in range(len(chunk_rows))]


def forward_kernel(meta, adj, *rest, blocks, ny, nx, pieces, chunk_rows):
    parts, rest = rest[: len(pieces)], rest[len(pieces) :]
    chunks = len(chunk_rows)
    outs = [rest[r * nx : (r + 1) * nx] for r in range(chunks)]
    head, nxt, col, acc, sems, products, out_sems = rest[chunks * nx :]
    nz = outs[0][0].shape[0]
    copies = []
    for n, (first, number) in enumerate(pieces):
        copies.append(
            pltpu.make_async_copy(parts[n], col.at[pl.ds(first, number)], sems.at[n])
        )
        copies[-1].start()
    link_tiles(lambda t: meta[1, t] // blocks, meta[2, 0], head, nxt, nx * nz)
    for copy in copies:
        copy.wait()
    my_y, my_c, my_x = meta[2, 1], meta[2, 2], meta[2, 3]

    def column_of(t):
        s = meta[0, t]
        holder = s // blocks
        rel_y = lax.rem(holder // 2 - my_y + ny, ny)
        rel_c = lax.rem(holder + my_c, 2)
        return col[(rel_y * 2 + rel_c) * blocks + lax.rem(s, blocks)]

    def pair(t, t2, has):
        second = adj[t2]
        second = jnp.where(has, second, jnp.zeros_like(second))
        left = jnp.concatenate([adj[t], second], axis=1)
        right = jnp.concatenate([column_of(t), column_of(t2)], axis=0)
        return jnp.dot(left, right, preferred_element_type=jnp.float32)

    def master(n, _):
        k = n // nz
        zi = lax.rem(n, nz)
        m = zi * nx + lax.rem(my_x + k, nx)

        @pl.when(head[m] < 0)
        def _():
            products[k, zi] = jnp.zeros(products.shape[2:], products.dtype)

        @pl.when(head[m] >= 0)
        def _():
            walk(head, nxt, m, pair, acc)
            products[k, zi] = acc[...].astype(products.dtype)

        return 0

    lax.fori_loop(0, nx * nz, master, 0)
    copies = []
    for r, at in enumerate(starts_of(chunk_rows)):
        for k in range(nx):
            copies.append(
                pltpu.make_async_copy(
                    products.at[k, :, pl.ds(at, chunk_rows[r])], outs[r][k], out_sems.at[len(copies)]
                )
            )
            copies[-1].start()
    for copy in copies:
        copy.wait()


def forward_products(meta, adj, parts, pieces, blocks, ny, nx, nz):
    tiles, size, _ = adj.shape
    width = parts[0].shape[-1]
    outs = pl.pallas_call(
        functools.partial(
            forward_kernel,
            blocks=blocks,
            ny=ny,
            nx=nx,
            pieces=pieces,
            chunk_rows=CHUNK_ROWS,
        ),
        out_shape=[
            jax.ShapeDtypeStruct((nz, rows, width), jnp.bfloat16)
            for rows in CHUNK_ROWS
            for _ in range(nx)
        ],
        in_specs=[SMEM, VMEM] + [HBM] * len(parts),
        out_specs=[HBM] * (nx * len(CHUNK_ROWS)),
        scratch_shapes=[
            pltpu.SMEM((nx * nz,), jnp.int32),
            pltpu.SMEM((tiles,), jnp.int32),
            pltpu.VMEM((2 * ny * blocks, size, width), jnp.bfloat16),
            pltpu.VMEM((size, width), jnp.float32),
            pltpu.SemaphoreType.DMA((len(parts),)),
            pltpu.VMEM((nx, nz, size, width), jnp.bfloat16),
            pltpu.SemaphoreType.DMA((nx * len(CHUNK_ROWS),)),
        ],
        compiler_params=pltpu.CompilerParams(vmem_limit_bytes=40 * 1024 * 1024),
        cost_estimate=pl.CostEstimate(
            flops=2 * tiles * size * size * width, transcendentals=0, bytes_accessed=12_000_000
        ),
        name="forward_products",
    )(meta, adj, *parts)
    return [outs[r * nx : (r + 1) * nx] for r in range(len(CHUNK_ROWS))]


def backward_kernel(meta, adj, *rest, blocks, ny, nx, flip, chunk_rows):
    chunks = len(chunk_rows)
    parts, rest = rest[: chunks * nx], rest[chunks * nx :]
    out, head, nxt, wanted, acc, sems = rest
    copies = []
    for r, at in enumerate(starts_of(chunk_rows)):
        for k in range(nx):
            n = r * nx + k
            copies.append(
                pltpu.make_async_copy(
                    parts[n], wanted.at[k, :, pl.ds(at, chunk_rows[r])], sems.at[n]
                )
            )
            copies[-1].start()
    link_tiles(lambda t: meta[0, t], meta[2, 0], head, nxt, 2 * ny * blocks)
    for copy in copies:
        copy.wait()
    my_y, my_x = meta[2, 1], meta[2, 3]
    half = lax.rem(meta[2, 2] + flip, 2)

    def rows_of(t):
        m = meta[1, t] // blocks
        return wanted[lax.rem(lax.rem(m, nx) - my_x + nx, nx), m // nx]

    def pair(t, t2, has):
        second = adj[t2]
        second = jnp.where(has, second, jnp.zeros_like(second))
        left = jnp.concatenate([adj[t], second], axis=0)
        right = jnp.concatenate([rows_of(t), rows_of(t2)], axis=0)
        return lax.dot_general(
            left, right, (((0,), (0,)), ((), ())), preferred_element_type=jnp.float32
        )

    def block(g, _):
        holder = lax.rem(my_y + g // blocks, ny) * 2 + half
        s = holder * blocks + lax.rem(g, blocks)

        @pl.when(head[s] < 0)
        def _():
            out[g] = jnp.zeros(out.shape[1:], out.dtype)

        @pl.when(head[s] >= 0)
        def _():
            walk(head, nxt, s, pair, acc)
            out[g] = acc[...].astype(out.dtype)

        return 0

    lax.fori_loop(0, ny * blocks, block, 0)


def backward_products(meta, adj, received, blocks, ny, flip):
    tiles, size, _ = adj.shape
    nx = len(received[0])
    nz, _, width = received[0][0].shape
    parts = [part for chunk in received for part in chunk]
    return pl.pallas_call(
        functools.partial(
            backward_kernel, blocks=blocks, ny=ny, nx=nx, flip=flip, chunk_rows=CHUNK_ROWS
        ),
        out_shape=jax.ShapeDtypeStruct((ny * blocks, size, width), jnp.bfloat16),
        in_specs=[SMEM, VMEM] + [HBM] * len(parts),
        out_specs=VMEM,
        scratch_shapes=[
            pltpu.SMEM((2 * ny * blocks,), jnp.int32),
            pltpu.SMEM((tiles,), jnp.int32),
            pltpu.VMEM((nx, nz, size, width), jnp.bfloat16),
            pltpu.VMEM((size, width), jnp.float32),
            pltpu.SemaphoreType.DMA((len(parts),)),
        ],
        compiler_params=pltpu.CompilerParams(vmem_limit_bytes=40 * 1024 * 1024),
        cost_estimate=pl.CostEstimate(
            flops=tiles * size * size * width, transcendentals=0, bytes_accessed=10_000_000
        ),
        name="backward_products",
    )(meta, adj, *parts)


def combine_kernel(asked, *refs, step):
    arrived, out = refs[:-1], refs[-1]
    base = pl.program_id(0) * step
    _, blocks, rows, width = out.shape
    half = width // 2

    def slab(n, _):
        at = pl.multiple_of(lax.rem(n, rows // 16) * 16, 16)
        z = n // (rows // 16)
        for left in (0, half):
            where = (z, pl.ds(at, 16), pl.ds(left, half))
            values = [ref[where].astype(jnp.float32) for ref in arrived]
            for j in range(blocks):
                total = jnp.where(asked[0, base + z] == j, values[0], 0.0)
                for k in range(1, len(values)):
                    total += jnp.where(asked[k, base + z] == j, values[k], 0.0)
                out[z, j, pl.ds(at, 16), pl.ds(left, half)] = total.astype(out.dtype)
        return 0

    lax.fori_loop(0, step * (rows // 16), slab, 0)


def combine(asked, arrived, blocks):
    nz, rows, width = arrived[0].shape
    step = 2
    return pl.pallas_call(
        functools.partial(combine_kernel, step=step),
        grid=(nz // step,),
        out_shape=jax.ShapeDtypeStruct((nz, blocks, rows, width), jnp.bfloat16),
        in_specs=[SMEM]
        + [pl.BlockSpec((step, rows, width), lambda z: (z, 0, 0))] * len(arrived),
        out_specs=pl.BlockSpec((step, blocks, rows, width), lambda z: (z, 0, 0, 0)),
        cost_estimate=pl.CostEstimate(
            flops=8 * len(arrived) * nz * rows * width,
            transcendentals=0,
            bytes_accessed=6 * nz * rows * width * 2,
        ),
        name="combine",
    )(asked, *arrived)


def pick_kernel(asked, held, *outs, step):
    base = pl.program_id(0) * step
    for z in range(step):
        for k, out in enumerate(outs):
            out[z] = held[z, asked[k, base + z]]


def pick(asked, held, nx):
    nz, blocks, rows, width = held.shape
    step = 2
    return pl.pallas_call(
        functools.partial(pick_kernel, step=step),
        grid=(nz // step,),
        out_shape=[jax.ShapeDtypeStruct((nz, rows, width), jnp.bfloat16)] * nx,
        in_specs=[SMEM, pl.BlockSpec((step, blocks, rows, width), lambda z: (z, 0, 0, 0))],
        out_specs=[pl.BlockSpec((step, rows, width), lambda z: (z, 0, 0))] * nx,
        cost_estimate=pl.CostEstimate(
            flops=nx * nz * rows * width,
            transcendentals=0,
            bytes_accessed=6 * nz * rows * width * 2,
        ),
        name="pick",
    )(asked, held)


def shifted(x, axis, by):
    n = lax.axis_size(axis)
    return lax.ppermute(x, axis, [(i, (i + by) % n) for i in range(n)])


def rolled(x, by):
    return lax.dynamic_slice_in_dim(jnp.concatenate([x, x], axis=0), by, x.shape[0], 0)


def summed_blocks(x, axis):
    ahead = rolled(x, lax.axis_index(axis))
    total = ahead[0].astype(jnp.float32)
    for k in range(1, x.shape[0]):
        total += shifted(ahead[k], axis, k).astype(jnp.float32)
    return total


def ring_of_four(x, split):
    left = shifted(x, "y", 1)
    right = shifted(x, "y", -1)
    far = [shifted(left[:split], "y", 1), shifted(right[split:], "y", -1)]
    own = [x, right, *far, left]
    return own, [shifted(part, "c", 1) for part in own]


def gather_kernel(place, *refs, ny, pieces):
    parts, (weight, bias, held, sems) = refs[: len(pieces)], refs[len(pieces) :]
    rows = weight.shape[0] // (2 * ny)
    copies = []
    for n, (rel_y, rel_c, first, number) in enumerate(pieces):
        slot = lax.rem(place[0] + rel_y, ny) * 2 + lax.rem(place[1] + rel_c, 2)
        copies.append(
            pltpu.make_async_copy(parts[n], held.at[slot, pl.ds(first, number)], sems.at[n])
        )
        copies[-1].start()
    for copy in copies:
        copy.wait()
    total = jnp.zeros(bias.shape, jnp.float32)
    for n in range(2 * ny):
        weight[n * rows : (n + 1) * rows] = held[n, :rows].astype(jnp.float32)
        total += held[n, rows : rows + 16].astype(jnp.float32)[:8]
    bias[...] = total


def gathered_grads(place, parts, pieces, ny, rows):
    padded, hidden = parts[0].shape
    return pl.pallas_call(
        functools.partial(gather_kernel, ny=ny, pieces=pieces),
        out_shape=[
            jax.ShapeDtypeStruct((2 * ny * rows, hidden), jnp.float32),
            jax.ShapeDtypeStruct((8, hidden), jnp.float32),
        ],
        in_specs=[SMEM] + [HBM] * len(parts),
        out_specs=[VMEM, VMEM],
        scratch_shapes=[
            pltpu.VMEM((2 * ny, padded, hidden), jnp.bfloat16),
            pltpu.SemaphoreType.DMA((len(parts),)),
        ],
        name="gather_grads",
    )(place, *parts)


def reduced_grads(weight_term, bias_term, place):
    feat, hidden = weight_term.shape
    ny, src = lax.axis_size("y"), lax.axis_size(SRC)
    nz, nx = lax.axis_size("z"), lax.axis_size("x")
    per_z = feat // src // nx // nz
    per_x = per_z * nz
    own = summed_blocks(weight_term.astype(jnp.bfloat16).reshape(src, feat // src, hidden), SRC)
    own = own.astype(jnp.bfloat16).reshape(nx, per_x, hidden)
    bias = bias_term.astype(jnp.bfloat16).reshape(nx, 1, hidden // nx)
    bias = jnp.pad(bias, ((0, 0), (0, 7), (0, hidden - hidden // nx)))
    own = summed_blocks(jnp.concatenate([own, bias], axis=1), "x").astype(jnp.bfloat16)
    bias = own[per_x, : hidden // nx].reshape(nz, 1, -1)
    bias = jnp.pad(bias, ((0, 0), (0, 0), (0, hidden - bias.shape[2])))
    lines = jnp.concatenate([own[:per_x].reshape(nz, per_z, hidden), bias], axis=1)
    arrived = lax.all_to_all(lines, "z", 0, 0, tiled=True)
    summed = jnp.sum(arrived.astype(jnp.float32), axis=0).astype(jnp.bfloat16)
    lines = lax.all_to_all(
        jnp.broadcast_to(summed[None], (nz, *summed.shape)), "z", 0, 0, tiled=True
    )
    mine = lines[:, :per_z].reshape(per_x, hidden)
    bias = lines[:, per_z, : hidden // nx // nz].reshape(1, hidden // nx)
    bias = jnp.pad(bias, ((0, 7), (0, hidden - hidden // nx)))
    mine = jnp.concatenate([mine, bias], axis=0)
    by_x = jnp.stack([mine] + [shifted(mine, "x", -k) for k in range(1, nx)])
    by_x = rolled(by_x, nx - place[2])
    mine = by_x[:, :per_x].reshape(nx * per_x, hidden)
    bias = by_x[:, per_x, : hidden // nx].reshape(1, hidden)
    mine = jnp.concatenate([mine, jnp.pad(bias, ((0, 15), (0, 0)))], axis=0)
    rows = nx * per_x
    split = rows // 2
    own, other = ring_of_four(mine, split)
    spans = (
        (0, 0, rows + 16),
        (1, 0, rows + 16),
        (2, 0, split),
        (2, split, rows + 16 - split),
        (3, 0, rows + 16),
    )
    pieces = tuple((y, c, first, number) for c in (0, 1) for y, first, number in spans)
    weight_grad, bias_grad = gathered_grads(place, own + other, pieces, ny, rows)
    return weight_grad, bias_grad[0]


def per_device(features, edge_tiles, tile_src, tile_dst, tile_count, weight, out_bias, out_grad):
    capacity, size = edge_tiles.shape[2:4]
    block_rows, feat_width = features.shape
    blocks = block_rows // size
    ny, nx, nz = lax.axis_size("y"), lax.axis_size("x"), lax.axis_size("z")
    masters = nx * nz
    my_y, my_c, my_x = lax.axis_index("y"), lax.axis_index("c"), lax.axis_index("x")
    place = jnp.stack([my_y, my_c, my_x]).astype(jnp.int32)
    adj = edge_tiles.reshape(capacity, size, size)
    src_ids = tile_src.reshape(capacity)
    dst_ids = tile_dst.reshape(capacity)
    count = tile_count.reshape(1)

    own, other = ring_of_four(features.reshape(blocks, size, feat_width), blocks // 2)
    firsts = ((0, blocks), (2, blocks), (4, blocks // 2), (4, blocks // 2), (6, blocks))
    pieces = []
    for at in (0, 1):
        for n, (rel, number) in enumerate(firsts):
            pieces.append(((rel + at) * blocks + (blocks // 2 if n == 3 else 0), number))

    own_line = jnp.concatenate([count, place, jnp.zeros((capacity - 4,), jnp.int32)])
    meta = jnp.stack([src_ids, dst_ids, own_line])
    alive = jnp.arange(capacity, dtype=jnp.int32) < count[0]
    routing = (dst_ids // blocks)[None, :] == jnp.arange(masters, dtype=jnp.int32)[:, None]
    inner = jnp.where(routing & alive[None, :], (dst_ids % blocks)[None, :], 0)
    wanted = jnp.max(inner, axis=1).reshape(nz, nx).T
    lines = jnp.broadcast_to(wanted[:, :, None], (nx, nz, 128))
    lines = rolled(lines, my_x)
    asked = [lines[0]] + [shifted(lines[k], "x", k) for k in range(1, nx)]
    asked = jnp.stack([line[:, 0] for line in asked])

    outgoing = forward_products(
        meta, adj, own + other, tuple(pieces), blocks, ny, nx, nz
    )

    grads = out_grad.reshape(blocks, size, -1)
    hidden, aggregates, pre_grads, bias_term, backs, received = [], [], [], 0.0, [], []
    for r, at in enumerate(starts_of(CHUNK_ROWS)):
        rows = CHUNK_ROWS[r]
        arrived = [outgoing[r][0]]
        arrived += [shifted(outgoing[r][k], "x", k) for k in range(1, nx)]
        if r > 1:
            arrived, _ = lax.optimization_barrier((arrived, backs[r - 2]))
        merged = combine(asked, arrived, blocks)
        aggregate = lax.all_to_all(
            merged.reshape(nz, blocks * rows, feat_width), "z", 0, 0, tiled=True
        )
        if r > 0:
            aggregate, _ = lax.optimization_barrier((aggregate, backs[r - 1]))
        aggregate = jnp.sum(aggregate.astype(jnp.float32), axis=0).astype(jnp.bfloat16)
        preact = jnp.dot(aggregate, weight, preferred_element_type=jnp.float32) + out_bias
        gate = jax.nn.sigmoid(preact)
        hidden.append((preact * gate).astype(jnp.bfloat16).reshape(blocks, rows, -1))
        grad_in = grads[:, at : at + rows].reshape(blocks * rows, -1)
        pre_grad = grad_in.astype(jnp.float32) * (gate * (1.0 + preact * (1.0 - gate)))
        pre_grad_b = pre_grad.astype(jnp.bfloat16)
        bias_term += jnp.sum(pre_grad, axis=0)
        aggregates.append(aggregate)
        pre_grads.append(pre_grad_b)
        back = lax.dot_general(
            pre_grad_b, weight, (((1,), (1,)), ((), ())), preferred_element_type=jnp.float32
        ).astype(jnp.bfloat16)
        backs.append(back)
    for r, rows in enumerate(CHUNK_ROWS):
        back = backs[r]
        if r < len(CHUNK_ROWS) - 1:
            held = lax.all_gather(back, "z", axis=0, tiled=True)
        else:
            held = lax.all_to_all(
                jnp.broadcast_to(back[None], (nz, *back.shape)), "z", 0, 0, tiled=True
            )
        chosen = pick(asked, held.reshape(nz, blocks, rows, feat_width), nx)
        received.append([chosen[0]] + [shifted(chosen[k], "x", -k) for k in range(1, nx)])

    weight_term = lax.dot_general(
        jnp.concatenate(aggregates, axis=0),
        jnp.concatenate(pre_grads, axis=0),
        (((0,), (0,)), ((), ())),
        preferred_element_type=jnp.float32,
    )
    weight_grad, bias_grad = reduced_grads(weight_term, bias_term, place)

    halves = []
    for flip in (1, 0):
        halves.append(backward_products(meta, adj, received, blocks, ny, flip))
    partner = shifted(halves[0], "c", 1)
    both = [
        halves[1][k * blocks : (k + 1) * blocks].astype(jnp.float32)
        + partner[k * blocks : (k + 1) * blocks].astype(jnp.float32)
        for k in range(ny)
    ]
    total = both[0]
    for k in range(1, ny):
        total += shifted(both[k].astype(jnp.bfloat16), "y", k).astype(jnp.float32)
    feature_grad = total.astype(jnp.bfloat16).reshape(block_rows, feat_width)
    hidden = jnp.concatenate(hidden, axis=1).reshape(block_rows, -1)
    return (hidden, feature_grad, weight_grad, bias_grad)


def solution(mesh):
    split = Mesh(mesh.devices.reshape(4, 2, 8, 4), ALL)
    in_specs = (
        P(ALL, None),
        P(SRC, DST, None, None, None),
        P(SRC, DST, None),
        P(SRC, DST, None),
        P(SRC, DST),
        P(),
        P(),
        P(ALL, None),
    )
    out_specs = (P(ALL, None), P(ALL, None), P(), P())
    return jax.shard_map(
        per_device, mesh=split, in_specs=in_specs, out_specs=out_specs, check_vma=False
    )
```

```python
import functools

import jax
import jax.numpy as jnp
from jax import lax
from jax.experimental import pallas as pl
from jax.experimental.pallas import tpu as pltpu
from jax.sharding import Mesh
from jax.sharding import PartitionSpec as P

SRC = ("y", "c")
DST = ("z", "x")
ALL = ("y", "c", "z", "x")
CHUNK_ROWS = (48, 48, 32)
RINGS = 1
SMEM = pl.BlockSpec(memory_space=pltpu.SMEM)
VMEM = pl.BlockSpec(memory_space=pltpu.VMEM)
HBM = pl.BlockSpec(memory_space=pltpu.HBM)


def link_tiles(key_of, count, head, nxt, groups):
    def clear(g, _):
        head[g] = -1
        return 0

    lax.fori_loop(0, groups, clear, 0)

    def push(t, _):
        g = key_of(t)
        nxt[t] = head[g]
        head[g] = t
        return 0

    lax.fori_loop(0, count, push, 0)


def walk(head, nxt, g, pair, acc):
    def one(t):
        t2 = nxt[t]
        has = t2 >= 0
        t2 = jnp.maximum(t2, 0)
        return pair(t, t2, has), jnp.where(has, nxt[t2], -1)

    value, t = one(head[g])
    acc[...] = value

    def more(t):
        value, t = one(t)
        acc[...] += value
        return t

    lax.while_loop(lambda t: t >= 0, more, t)


def starts_of(chunk_rows):
    return [sum(chunk_rows[:r]) for r in range(len(chunk_rows))]


def forward_kernel(meta, adj, *rest, blocks, ny, nx, pieces, chunk_rows):
    parts, rest = rest[: len(pieces)], rest[len(pieces) :]
    chunks = len(chunk_rows)
    outs = [rest[r * nx : (r + 1) * nx] for r in range(chunks)]
    head, nxt, col, acc, products, out_sems = rest[chunks * nx :]
    nz = outs[0][0].shape[0]
    link_tiles(lambda t: meta[1, t] // blocks, meta[2, 0], head, nxt, nx * nz)
    for n, (first, number) in enumerate(pieces):
        col[first : first + number] = parts[n][...]
    my_y, my_c, my_x = meta[2, 1], meta[2, 2], meta[2, 3]

    def column_of(t):
        s = meta[0, t]
        holder = s // blocks
        rel_y = lax.rem(holder // 2 - my_y + ny, ny)
        rel_c = lax.rem(holder + my_c, 2)
        return col[(rel_y * 2 + rel_c) * blocks + lax.rem(s, blocks)]

    def pair(t, t2, has):
        second = adj[t2]
        second = jnp.where(has, second, jnp.zeros_like(second))
        left = jnp.concatenate([adj[t], second], axis=1)
        right = jnp.concatenate([column_of(t), column_of(t2)], axis=0)
        return jnp.dot(left, right, preferred_element_type=jnp.float32)

    def master(n, _):
        k = n // nz
        zi = lax.rem(n, nz)
        m = zi * nx + lax.rem(my_x + k, nx)

        @pl.when(head[m] < 0)
        def _():
            products[k, zi] = jnp.zeros(products.shape[2:], products.dtype)

        @pl.when(head[m] >= 0)
        def _():
            walk(head, nxt, m, pair, acc)
            products[k, zi] = acc[...].astype(products.dtype)

        return 0

    lax.fori_loop(0, nx * nz, master, 0)
    copies = []
    for r, at in enumerate(starts_of(chunk_rows)):
        for k in range(nx):
            copies.append(
                pltpu.make_async_copy(
                    products.at[k, :, pl.ds(at, chunk_rows[r])], outs[r][k], out_sems.at[len(copies)]
                )
            )
            copies[-1].start()
    for copy in copies:
        copy.wait()


def forward_products(meta, adj, parts, pieces, blocks, ny, nx, nz):
    tiles, size, _ = adj.shape
    width = parts[0].shape[-1]
    outs = pl.pallas_call(
        functools.partial(
            forward_kernel,
            blocks=blocks,
            ny=ny,
            nx=nx,
            pieces=pieces,
            chunk_rows=CHUNK_ROWS,
        ),
        out_shape=[
            jax.ShapeDtypeStruct((nz, rows, width), jnp.bfloat16)
            for rows in CHUNK_ROWS
            for _ in range(nx)
        ],
        in_specs=[SMEM, VMEM] + [VMEM] * len(parts),
        out_specs=[HBM] * (nx * len(CHUNK_ROWS)),
        scratch_shapes=[
            pltpu.SMEM((nx * nz,), jnp.int32),
            pltpu.SMEM((tiles,), jnp.int32),
            pltpu.VMEM((2 * ny * blocks, size, width), jnp.bfloat16),
            pltpu.VMEM((size, width), jnp.float32),
            pltpu.VMEM((nx, nz, size, width), jnp.bfloat16),
            pltpu.SemaphoreType.DMA((nx * len(CHUNK_ROWS),)),
        ],
        compiler_params=pltpu.CompilerParams(vmem_limit_bytes=40 * 1024 * 1024),
        cost_estimate=pl.CostEstimate(
            flops=2 * tiles * size * size * width, transcendentals=0, bytes_accessed=12_000_000
        ),
        name="forward_products",
    )(meta, adj, *parts)
    return [outs[r * nx : (r + 1) * nx] for r in range(len(CHUNK_ROWS))]


def backward_kernel(meta, adj, *rest, blocks, ny, nx, chunk_rows):
    chunks = len(chunk_rows)
    parts, (out, head, nxt, wanted, acc) = rest[: chunks * nx], rest[chunks * nx :]
    half = out.shape[1]
    link_tiles(lambda t: meta[0, t], meta[2, 0], head, nxt, 2 * half)
    for r, at in enumerate(starts_of(chunk_rows)):
        for k in range(nx):
            part = parts[r * nx + k]

            def place_rows(z, _):
                wanted[k, z, at : at + chunk_rows[r]] = part[z]
                return 0

            lax.fori_loop(0, part.shape[0], place_rows, 0)
    my_y, my_c, my_x = meta[2, 1], meta[2, 2], meta[2, 3]

    def rows_of(t):
        m = meta[1, t] // blocks
        return wanted[lax.rem(lax.rem(m, nx) - my_x + nx, nx), m // nx]

    def pair(t, t2, has):
        second = adj[t2]
        second = jnp.where(has, second, jnp.zeros_like(second))
        left = jnp.concatenate([adj[t], second], axis=0)
        right = jnp.concatenate([rows_of(t), rows_of(t2)], axis=0)
        return lax.dot_general(
            left, right, (((0,), (0,)), ((), ())), preferred_element_type=jnp.float32
        )

    def block(n, _):
        flip = n // half
        g = lax.rem(n, half)
        holder = lax.rem(my_y + g // blocks, ny) * 2 + lax.rem(my_c + flip, 2)
        s = holder * blocks + lax.rem(g, blocks)

        @pl.when(head[s] < 0)
        def _():
            out[flip, g] = jnp.zeros(out.shape[2:], out.dtype)

        @pl.when(head[s] >= 0)
        def _():
            walk(head, nxt, s, pair, acc)
            out[flip, g] = acc[...].astype(out.dtype)

        return 0

    lax.fori_loop(0, 2 * half, block, 0)


def backward_products(meta, adj, received, blocks, ny):
    tiles, size, _ = adj.shape
    nx = len(received[0])
    nz, _, width = received[0][0].shape
    parts = [part for chunk in received for part in chunk]
    return pl.pallas_call(
        functools.partial(backward_kernel, blocks=blocks, ny=ny, nx=nx, chunk_rows=CHUNK_ROWS),
        out_shape=jax.ShapeDtypeStruct((2, ny * blocks, size, width), jnp.bfloat16),
        in_specs=[SMEM, VMEM] + [VMEM] * len(parts),
        out_specs=VMEM,
        scratch_shapes=[
            pltpu.SMEM((2 * ny * blocks,), jnp.int32),
            pltpu.SMEM((tiles,), jnp.int32),
            pltpu.VMEM((nx, nz, size, width), jnp.bfloat16),
            pltpu.VMEM((size, width), jnp.float32),
        ],
        compiler_params=pltpu.CompilerParams(vmem_limit_bytes=40 * 1024 * 1024),
        cost_estimate=pl.CostEstimate(
            flops=2 * tiles * size * size * width, transcendentals=0, bytes_accessed=12_000_000
        ),
        name="backward_products",
    )(meta, adj, *parts)


def combine_kernel(asked, *refs, step):
    arrived, out = refs[:-1], refs[-1]
    base = pl.program_id(0) * step
    _, blocks, rows, width = out.shape
    half = width // 2

    def slab(n, _):
        at = pl.multiple_of(lax.rem(n, rows // 16) * 16, 16)
        z = n // (rows // 16)
        for left in (0, half):
            where = (z, pl.ds(at, 16), pl.ds(left, half))
            values = [ref[where].astype(jnp.float32) for ref in arrived]
            for j in range(blocks):
                total = jnp.where(asked[0, base + z] == j, values[0], 0.0)
                for k in range(1, len(values)):
                    total += jnp.where(asked[k, base + z] == j, values[k], 0.0)
                out[z, j, pl.ds(at, 16), pl.ds(left, half)] = total.astype(out.dtype)
        return 0

    lax.fori_loop(0, step * (rows // 16), slab, 0)


def combine(asked, arrived, blocks):
    nz, rows, width = arrived[0].shape
    step = 2
    return pl.pallas_call(
        functools.partial(combine_kernel, step=step),
        grid=(nz // step,),
        out_shape=jax.ShapeDtypeStruct((nz, blocks, rows, width), jnp.bfloat16),
        in_specs=[SMEM]
        + [pl.BlockSpec((step, rows, width), lambda z: (z, 0, 0))] * len(arrived),
        out_specs=pl.BlockSpec((step, blocks, rows, width), lambda z: (z, 0, 0, 0)),
        cost_estimate=pl.CostEstimate(
            flops=8 * len(arrived) * nz * rows * width,
            transcendentals=0,
            bytes_accessed=6 * nz * rows * width * 2,
        ),
        name="combine",
    )(asked, *arrived)


def pick_kernel(asked, held, *outs, step):
    base = pl.program_id(0) * step
    for z in range(step):
        for k, out in enumerate(outs):
            out[z] = held[z, asked[k, base + z]]


def pick(asked, held, nx):
    nz, blocks, rows, width = held.shape
    step = 2
    return pl.pallas_call(
        functools.partial(pick_kernel, step=step),
        grid=(nz // step,),
        out_shape=[jax.ShapeDtypeStruct((nz, rows, width), jnp.bfloat16)] * nx,
        in_specs=[SMEM, pl.BlockSpec((step, blocks, rows, width), lambda z: (z, 0, 0, 0))],
        out_specs=[pl.BlockSpec((step, rows, width), lambda z: (z, 0, 0))] * nx,
        cost_estimate=pl.CostEstimate(
            flops=nx * nz * rows * width,
            transcendentals=0,
            bytes_accessed=6 * nz * rows * width * 2,
        ),
        name="pick",
    )(asked, held)


def pick_ring_kernel(meta, asked, *refs):
    outs, parts = refs[8:], refs[:8]
    for n, part in enumerate(parts):
        z = lax.rem(meta[2, 4] + n, len(parts))
        for k, out in enumerate(outs):
            out[z] = part[asked[k, z]]


def pick_ring(meta, asked, parts, nx):
    _, rows, width = parts[0].shape
    return pl.pallas_call(
        pick_ring_kernel,
        out_shape=[jax.ShapeDtypeStruct((len(parts), rows, width), jnp.bfloat16)] * nx,
        in_specs=[SMEM, SMEM] + [VMEM] * len(parts),
        out_specs=[VMEM] * nx,
        cost_estimate=pl.CostEstimate(
            flops=nx * len(parts) * rows * width,
            transcendentals=0,
            bytes_accessed=12 * len(parts) * rows * width,
        ),
        name="pick_ring",
    )(meta, asked, *parts)


def ring_of_eight(x):
    up, down = [x], [x]
    for step in range(4):
        up.append(shifted(up[-1], "z", 1))
        if step < 3:
            down.append(shifted(down[-1], "z", -1))
    return down + up[:0:-1]


def shifted(x, axis, by):
    n = lax.axis_size(axis)
    return lax.ppermute(x, axis, [(i, (i + by) % n) for i in range(n)])


def rolled(x, by):
    return lax.dynamic_slice_in_dim(jnp.concatenate([x, x], axis=0), by, x.shape[0], 0)


def summed_blocks(x, axis):
    ahead = rolled(x, lax.axis_index(axis))
    total = ahead[0].astype(jnp.float32)
    for k in range(1, x.shape[0]):
        total += shifted(ahead[k], axis, k).astype(jnp.float32)
    return total


def ring_of_four(x, split):
    left = shifted(x, "y", 1)
    right = shifted(x, "y", -1)
    far = [shifted(left[:split], "y", 1), shifted(right[split:], "y", -1)]
    own = [x, right, *far, left]
    return own, [shifted(part, "c", 1) for part in own]


def gather_kernel(place, *refs, ny, pieces):
    parts, (weight, bias, held) = refs[: len(pieces)], refs[len(pieces) :]
    rows = weight.shape[1]
    for n, (rel_y, rel_c, first, number) in enumerate(pieces):
        slot = lax.rem(place[0] + rel_y, ny) * 2 + lax.rem(place[1] + rel_c, 2)
        held[slot, first : first + number] = parts[n][...]
    bias[...] = jnp.zeros(bias.shape, jnp.float32)

    def widen(n, _):
        weight[n] = held[n, :rows].astype(jnp.float32)
        bias[...] += held[n, rows : rows + 16].astype(jnp.float32)[:8]
        return 0

    lax.fori_loop(0, 2 * ny, widen, 0)


def gathered_grads(place, parts, pieces, ny, rows):
    padded, hidden = parts[0].shape
    return pl.pallas_call(
        functools.partial(gather_kernel, ny=ny, pieces=pieces),
        out_shape=[
            jax.ShapeDtypeStruct((2 * ny, rows, hidden), jnp.float32),
            jax.ShapeDtypeStruct((8, hidden), jnp.float32),
        ],
        in_specs=[SMEM] + [VMEM] * len(parts),
        out_specs=[VMEM, VMEM],
        scratch_shapes=[
            pltpu.VMEM((2 * ny, padded, hidden), jnp.bfloat16),
        ],
        name="gather_grads",
    )(place, *parts)


def reduced_grads(weight_term, bias_term, place):
    feat, hidden = weight_term.shape
    ny, src = lax.axis_size("y"), lax.axis_size(SRC)
    nz, nx = lax.axis_size("z"), lax.axis_size("x")
    per_z = feat // src // nx // nz
    per_x = per_z * nz
    own = summed_blocks(weight_term.astype(jnp.bfloat16).reshape(src, feat // src, hidden), SRC)
    own = own.astype(jnp.bfloat16).reshape(nx, per_x, hidden)
    bias = bias_term.astype(jnp.bfloat16).reshape(nx, 1, hidden // nx)
    bias = jnp.pad(bias, ((0, 0), (0, 7), (0, hidden - hidden // nx)))
    own = summed_blocks(jnp.concatenate([own, bias], axis=1), "x").astype(jnp.bfloat16)
    bias = own[per_x, : hidden // nx].reshape(nz, 1, -1)
    bias = jnp.pad(bias, ((0, 0), (0, 0), (0, hidden - bias.shape[2])))
    lines = jnp.concatenate([own[:per_x].reshape(nz, per_z, hidden), bias], axis=1)
    arrived = lax.all_to_all(lines, "z", 0, 0, tiled=True)
    summed = jnp.sum(arrived.astype(jnp.float32), axis=0).astype(jnp.bfloat16)
    lines = lax.all_to_all(
        jnp.broadcast_to(summed[None], (nz, *summed.shape)), "z", 0, 0, tiled=True
    )
    mine = lines[:, :per_z].reshape(per_x, hidden)
    bias = lines[:, per_z, : hidden // nx // nz].reshape(1, hidden // nx)
    bias = jnp.pad(bias, ((0, 7), (0, hidden - hidden // nx)))
    mine = jnp.concatenate([mine, bias], axis=0)
    by_x = jnp.stack([mine] + [shifted(mine, "x", -k) for k in range(1, nx)])
    by_x = rolled(by_x, nx - place[2])
    mine = by_x[:, :per_x].reshape(nx * per_x, hidden)
    bias = by_x[:, per_x, : hidden // nx].reshape(1, hidden)
    mine = jnp.concatenate([mine, jnp.pad(bias, ((0, 15), (0, 0)))], axis=0)
    rows = nx * per_x
    split = rows // 2
    own, other = ring_of_four(mine, split)
    spans = (
        (0, 0, rows + 16),
        (1, 0, rows + 16),
        (2, 0, split),
        (2, split, rows + 16 - split),
        (3, 0, rows + 16),
    )
    pieces = tuple((y, c, first, number) for c in (0, 1) for y, first, number in spans)
    weight_grad, bias_grad = gathered_grads(place, own + other, pieces, ny, rows)
    return weight_grad.reshape(feat, hidden), bias_grad[0]


def per_device(features, edge_tiles, tile_src, tile_dst, tile_count, weight, out_bias, out_grad):
    capacity, size = edge_tiles.shape[2:4]
    block_rows, feat_width = features.shape
    blocks = block_rows // size
    ny, nx, nz = lax.axis_size("y"), lax.axis_size("x"), lax.axis_size("z")
    masters = nx * nz
    my_y, my_c, my_x = lax.axis_index("y"), lax.axis_index("c"), lax.axis_index("x")
    place = jnp.stack([my_y, my_c, my_x, lax.axis_index("z")]).astype(jnp.int32)
    adj = edge_tiles.reshape(capacity, size, size)
    src_ids = tile_src.reshape(capacity)
    dst_ids = tile_dst.reshape(capacity)
    count = tile_count.reshape(1)

    own, other = ring_of_four(features.reshape(blocks, size, feat_width), blocks // 2)
    firsts = ((0, blocks), (2, blocks), (4, blocks // 2), (4, blocks // 2), (6, blocks))
    pieces = []
    for at in (0, 1):
        for n, (rel, number) in enumerate(firsts):
            pieces.append(((rel + at) * blocks + (blocks // 2 if n == 3 else 0), number))

    own_line = jnp.concatenate([count, place, jnp.zeros((capacity - 5,), jnp.int32)])
    meta = jnp.stack([src_ids, dst_ids, own_line])
    alive = jnp.arange(capacity, dtype=jnp.int32) < count[0]
    routing = (dst_ids // blocks)[None, :] == jnp.arange(masters, dtype=jnp.int32)[:, None]
    inner = jnp.where(routing & alive[None, :], (dst_ids % blocks)[None, :], 0)
    wanted = jnp.max(inner, axis=1).reshape(nz, nx).T
    lines = jnp.broadcast_to(wanted[:, :, None], (nx, nz, 128))
    lines = rolled(lines, my_x)
    asked = [lines[0]] + [shifted(lines[k], "x", k) for k in range(1, nx)]
    asked = jnp.stack([line[:, 0] for line in asked])

    outgoing = forward_products(
        meta, adj, own + other, tuple(pieces), blocks, ny, nx, nz
    )

    grads = out_grad.reshape(blocks, size, -1)
    hidden, aggregates, pre_grads, bias_term, backs, received = [], [], [], 0.0, [], []
    for r, at in enumerate(starts_of(CHUNK_ROWS)):
        rows = CHUNK_ROWS[r]
        arrived = [outgoing[r][0]]
        arrived += [shifted(outgoing[r][k], "x", k) for k in range(1, nx)]
        if r > 1:
            arrived, _ = lax.optimization_barrier((arrived, backs[r - 2]))
        merged = combine(asked, arrived, blocks)
        aggregate = lax.all_to_all(
            merged.reshape(nz, blocks * rows, feat_width), "z", 0, 0, tiled=True
        )
        if r > 0:
            aggregate, _ = lax.optimization_barrier((aggregate, backs[r - 1]))
        aggregate = jnp.sum(aggregate.astype(jnp.float32), axis=0).astype(jnp.bfloat16)
        preact = jnp.dot(aggregate, weight, preferred_element_type=jnp.float32) + out_bias
        gate = jax.nn.sigmoid(preact)
        hidden.append((preact * gate).astype(jnp.bfloat16).reshape(blocks, rows, -1))
        grad_in = grads[:, at : at + rows].reshape(blocks * rows, -1)
        pre_grad = grad_in.astype(jnp.float32) * (gate * (1.0 + preact * (1.0 - gate)))
        pre_grad_b = pre_grad.astype(jnp.bfloat16)
        bias_term += jnp.sum(pre_grad, axis=0)
        aggregates.append(aggregate)
        pre_grads.append(pre_grad_b)
        back = lax.dot_general(
            pre_grad_b, weight, (((1,), (1,)), ((), ())), preferred_element_type=jnp.float32
        ).astype(jnp.bfloat16)
        backs.append(back)
    for r, rows in enumerate(CHUNK_ROWS):
        back = backs[r]
        if r < RINGS:
            parts = ring_of_eight(back.reshape(blocks, rows, feat_width))
            chosen = pick_ring(meta, asked, parts, nx)
        else:
            held = lax.all_to_all(
                jnp.broadcast_to(back[None], (nz, *back.shape)), "z", 0, 0, tiled=True
            )
            chosen = pick(asked, held.reshape(nz, blocks, rows, feat_width), nx)
        received.append([chosen[0]] + [shifted(chosen[k], "x", -k) for k in range(1, nx)])

    weight_term = lax.dot_general(
        jnp.concatenate(aggregates, axis=0),
        jnp.concatenate(pre_grads, axis=0),
        (((0,), (0,)), ((), ())),
        preferred_element_type=jnp.float32,
    )
    weight_grad, bias_grad = reduced_grads(weight_term, bias_term, place)

    halves = backward_products(meta, adj, received, blocks, ny)
    partner = shifted(halves[1], "c", 1)
    both = [
        halves[0, k * blocks : (k + 1) * blocks].astype(jnp.float32)
        + partner[k * blocks : (k + 1) * blocks].astype(jnp.float32)
        for k in range(ny)
    ]
    total = both[0]
    for k in range(1, ny):
        total += shifted(both[k].astype(jnp.bfloat16), "y", k).astype(jnp.float32)
    feature_grad = total.astype(jnp.bfloat16).reshape(block_rows, feat_width)
    hidden = jnp.concatenate(hidden, axis=1).reshape(block_rows, -1)
    return (hidden, feature_grad, weight_grad, bias_grad)


def solution(mesh):
    split = Mesh(mesh.devices.reshape(4, 2, 8, 4), ALL)
    in_specs = (
        P(ALL, None),
        P(SRC, DST, None, None, None),
        P(SRC, DST, None),
        P(SRC, DST, None),
        P(SRC, DST),
        P(),
        P(),
        P(ALL, None),
    )
    out_specs = (P(ALL, None), P(ALL, None), P(), P())
    return jax.shard_map(
        per_device, mesh=split, in_specs=in_specs, out_specs=out_specs, check_vma=False
    )
```
